32 devices in a mesh: row: 4 (over y, x), col: 4 (over z), depth: 2 (over core).
Axes of the slice: x: 2, y: 2, z: 4, core: 2. Of those that a mesh axis runs over, the one named last changes fastest.
Arguments:
- halves: bfloat16 [2, 8192, 16384], P(None, 'row', ('col', 'depth')), may hold values from -6 to 6
- spectrum: float32 [2, 16384], P(None, ('col', 'depth')), as said below
- wanted: int32 [4096], P('col'), may hold values from 0 to 32766, as said below
- fraction: float32 [4096], P('col'), may hold values from 0.05 to 0.95
Outputs:
- eigvec: float32 [2, 8192, 4096], P(None, 'row', ('col', 'depth'))
The draws below stay inside these ranges and needn't reach their ends.
Inputs may be any that keep to these rules, and one draw needn't show every extreme that they name: Read in the order spectrum[0,0], spectrum[1,0], spectrum[0,1], spectrum[1,1], ... the values rise strictly, each by more than 0.05 over the one before. `wanted`: distinct positions in that merged order of the 32768 eigenvalues.
All inputs are finite; a program needn't handle non-finite values.
Results may differ from the reference program's by a relative error of at most 0.0029.
Values may be sent and summed in bfloat16 or wider, within the bound.
A program may use at most 192 MiB of HBM per device.

```python
import math
import jax
import jax.numpy as jnp
from jax import lax

H = 16384
R = 8192
K = 4096


def draw_halves(key, part):
    noise_key = jax.random.fold_in(key, 11)
    random_part = jnp.clip(jax.random.normal(noise_key, (2, R, H), jnp.float32), -6.0, 6.0)
    values = random_part
    return values.astype(jnp.bfloat16)


def draw_spectrum(key, part):
    gaps = jnp.exp(jax.random.uniform(key, (2 * H,), jnp.float32, math.log(0.5), math.log(2.0)))
    ordered = jnp.cumsum(gaps)
    ordered = ordered - 0.5 * ordered[-1]
    return ordered.reshape(H, 2).T.astype(jnp.float32)


def draw_wanted(key, part):
    return jax.random.permutation(key, 2 * H - 1)[:K].astype(jnp.int32)


def level_of(key, extent, pieces, low, top_value):
    gain = 1.0
    for position, blocks in pieces:
        draws = jax.random.uniform(jax.random.fold_in(jax.random.fold_in(key, 6), position), (blocks,), jnp.float32, low / len(pieces), top_value / len(pieces))
        gain = gain * jnp.repeat(jnp.exp(draws), extent[position] // blocks).reshape((-1,) + (1,) * (len(extent) - 1 - position))
    return gain


def setup_inputs(seed: int = 0) -> dict:
    arg_keys = jax.random.split(jax.random.key(seed), 5)
    return {
        "halves": draw_halves(jax.random.fold_in(arg_keys[4], 71), 0),
        "spectrum": draw_spectrum(jax.random.fold_in(arg_keys[4], 71), 0),
        "wanted": draw_wanted(jax.random.fold_in(arg_keys[4], 71), 0),
        "fraction": jnp.clip(0.05 + 0.9 * jax.random.uniform(arg_keys[3], (K,), jnp.float32) ** level_of(arg_keys[3], (K,), ((0, 4),), -0.2, 0.2), 0.05, 0.95),
    }


def root_terms(spectrum, wanted):
    ordered = jnp.stack([spectrum[0], spectrum[1]], axis=1).reshape(-1)
    lower = jnp.take(ordered, wanted)
    upper = jnp.take(ordered, wanted + 1)
    return (lower, upper - lower)

def reference(halves, spectrum, wanted, fraction):
    seam = jnp.stack([halves[0, R - 1], halves[1, 0]]).astype(jnp.float32)
    lower, width = root_terms(spectrum, wanted)
    block = math.gcd(K, 512)
    count = K // block

    def one(index):
        start = (index * block).astype(jnp.int32)
        low = lax.dynamic_slice_in_dim(lower, start, block)
        wid = lax.dynamic_slice_in_dim(width, start, block)
        frc = lax.dynamic_slice_in_dim(fraction, start, block)
        cauchy = seam[:, :, None] / (spectrum[:, :, None] - low[None, None, :] - frc[None, None, :] * wid[None, None, :])
        norms = jnp.sqrt(lax.optimization_barrier(jnp.sum(cauchy * cauchy, axis=(0, 1))))
        rounded = cauchy.astype(jnp.bfloat16)
        first = jnp.dot(halves[0], rounded[0], preferred_element_type=jnp.float32)
        second = jnp.dot(halves[1], rounded[1], preferred_element_type=jnp.float32)
        return jnp.stack([first, second]) / norms[None, None, :]
    result = lax.map(one, jnp.arange(count).astype(jnp.int32))
    return jnp.transpose(result, (1, 2, 0, 3)).reshape(2, R, K)
```

```python
import functools
import math

import jax
import jax.numpy as jnp
from jax import lax
from jax.experimental import pallas as pl
from jax.experimental.pallas import tpu as pltpu
from jax.sharding import PartitionSpec as P


def product_kernel(own_ref, par_ref, roots_ref, line_ref, out_ref, block_ref):
    inner = block_ref.shape[0]
    half = inner // 2
    step = math.gcd(inner, 64)

    @pl.when(pl.program_id(0) == 0)
    def _():
        lower = roots_ref[0:1, :]
        shift = roots_ref[1:2, :]

        def one(i, carry):
            rows = pl.ds(pl.multiple_of(i * step, step), step)
            value = line_ref[rows, 0:1]
            seam = line_ref[rows, 1:2]
            gap = (value - lower) - shift
            guess = pl.reciprocal(gap, approx=True)
            inverse = guess + guess * (1.0 - gap * guess)
            block_ref[rows, :] = (seam * inverse).astype(jnp.bfloat16)
            return carry

        lax.fori_loop(0, inner // step, one, 0)

    first = jnp.dot(own_ref[...], block_ref[0:half, :], preferred_element_type=jnp.float32)
    second = jnp.dot(par_ref[...], block_ref[half:inner, :], preferred_element_type=jnp.float32)
    out_ref[...] = (first + second).astype(out_ref.dtype)


def product(side, own, partner, roots, lines, dtype):
    rows = own.shape[1]
    half = own.shape[2]
    cols = roots.shape[1]
    tile = math.gcd(rows, 256)
    return pl.pallas_call(
        product_kernel,
        grid=(rows // tile,),
        in_specs=[
            pl.BlockSpec((None, tile, half), lambda i: (side, i, 0)),
            pl.BlockSpec((None, tile, half), lambda i: (side, i, 0)),
            pl.BlockSpec((2, cols), lambda i: (0, 0)),
            pl.BlockSpec((None, 2 * half, 2), lambda i: (side, 0, 0)),
        ],
        out_specs=pl.BlockSpec((tile, cols), lambda i: (i, 0)),
        out_shape=jax.ShapeDtypeStruct((rows, cols), dtype),
        scratch_shapes=[pltpu.VMEM((2 * half, cols), jnp.bfloat16)],
        cost_estimate=pl.CostEstimate(
            flops=4 * rows * half * cols,
            bytes_accessed=4 * rows * half + 4 * rows * cols,
            transcendentals=2 * half * cols,
        ),
        compiler_params=pltpu.CompilerParams(dimension_semantics=("arbitrary",)),
    )(own, partner, roots, lines)


def combine_kernel(count, *refs):
    own_ref = refs[0]
    norm_ref = refs[1 + count]
    out_ref = refs[-1]
    total = own_ref[...]
    for k in range(count):
        total = total + refs[1 + k][...].astype(jnp.float32)
    out_ref[...] = total / norm_ref[...]


def combine(side, own, parts, norms, whole):
    rows, cols = own.shape
    tile = math.gcd(rows, 256)
    count = len(parts)
    block = pl.BlockSpec((tile, cols), lambda i: (i, 0))
    operands = [own, *parts, norms]
    in_specs = [block] * (1 + count) + [pl.BlockSpec((1, cols), lambda i: (0, 0))]
    aliases = {}
    if whole is not None:
        aliases = {len(operands): 0}
        operands.append(whole)
        in_specs.append(pl.BlockSpec(memory_space=pl.ANY))
    return pl.pallas_call(
        functools.partial(combine_kernel, count),
        grid=(rows // tile,),
        in_specs=in_specs,
        out_specs=pl.BlockSpec((None, tile, cols), lambda i: (side, i, 0)),
        out_shape=jax.ShapeDtypeStruct((2, rows, cols), jnp.float32),
        input_output_aliases=aliases,
        cost_estimate=pl.CostEstimate(
            flops=(2 + count) * rows * cols, bytes_accessed=(8 + 2 * count) * rows * cols, transcendentals=0
        ),
        compiler_params=pltpu.CompilerParams(dimension_semantics=("arbitrary",)),
    )(*operands)


def look_up(table, row, lane):
    pick = (row[:, None] == lax.broadcasted_iota(jnp.int32, (1, table.shape[0]), 1)).astype(jnp.float32)
    lines = jnp.dot(pick, table, precision=lax.Precision.HIGHEST, preferred_element_type=jnp.float32)
    lanes = lax.broadcasted_iota(jnp.int32, (1, table.shape[1]), 1)
    return jnp.sum(jnp.where(lane[:, None] == lanes, lines, 0.0), axis=1)


def body(halves, spectrum, wanted, fraction):
    ncols = lax.axis_size("col")
    ndepth = lax.axis_size("depth")
    nrow = lax.axis_size("row")
    col = lax.axis_index("col")
    layer = lax.axis_index("depth")
    rows_here = halves.shape[1]
    width_here = halves.shape[2]
    kcol = wanted.shape[0]
    share = kcol // ndepth

    partner = lax.ppermute(halves, "depth", [(0, 1), (1, 0)])

    edges = jnp.stack([halves[0, rows_here - 1], halves[1, 0]])
    edges = lax.all_gather(edges, "row", axis=0, tiled=False)
    seam = jnp.stack([edges[nrow - 1, 0], edges[0, 1]]).astype(jnp.float32)

    lanes = math.gcd(width_here, 128)
    flat = jnp.concatenate(
        [spectrum.reshape(-1), seam.reshape(-1), wanted.astype(jnp.float32), fraction]
    )
    flat = lax.all_gather(flat, ("col", "depth"), axis=0, tiled=False)
    pieces = jnp.split(flat, [2 * width_here, 4 * width_here, 4 * width_here + kcol], axis=1)
    values, seams, position, frac = pieces
    table = values.reshape(-1, lanes)
    position = position.reshape(ncols, ndepth, kcol)[:, 0]
    frac = frac.reshape(ncols, ndepth, kcol)[:, 0]
    position = lax.dynamic_slice_in_dim(position, layer * share, share, axis=1).reshape(-1).astype(jnp.int32)
    frac = lax.dynamic_slice_in_dim(frac, layer * share, share, axis=1)

    def ordered(where):
        index = where // 2
        within = index % width_here
        row = ((index // width_here) * 2 + where % 2) * (width_here // lanes) + within // lanes
        return look_up(table, row, within % lanes).reshape(ncols, share)

    lower = ordered(position)
    shift = frac * (ordered(position + 1) - lower)
    roots = jnp.stack([lower, shift], axis=1)

    def near(full):
        full = full.reshape(ncols, ndepth, 2, width_here)
        full = lax.dynamic_index_in_dim(full, col, 0, keepdims=False)
        full = jnp.where(layer == 0, full, full[::-1])
        return jnp.transpose(full, (1, 0, 2)).reshape(2, ndepth * width_here)

    lines = jnp.stack([near(values), near(seams)], axis=2)

    def step(chunk, after=None, dtype=jnp.bfloat16):
        mine = lax.dynamic_index_in_dim(roots, chunk, 0, keepdims=False)
        if after is not None:
            mine, after = lax.optimization_barrier((mine, after))
        return [product(side, halves, partner, mine, lines, dtype) for side in range(2)]

    def wide(x):
        return x.astype(jnp.float32)

    def send(xs, moves):
        return [lax.ppermute(x, "col", moves) for x in xs]

    if ncols == 4:
        edge = (col == 0) | (col == 3)

        def choose(options):
            return jnp.take(jnp.array(options, jnp.int32), col)

        far = step(choose([3, 2, 1, 0]))
        got_edge = send(far, [(0, 1), (3, 2)])
        got_mid = send(far, [(1, 2), (2, 1)])
        two = step(choose([2, 3, 0, 1]))
        relay = [
            jnp.where(edge, t, (wide(t) + wide(x)).astype(jnp.bfloat16)) for t, x in zip(two, got_edge)
        ]
        got_two = send(relay, [(0, 2), (1, 3), (2, 0), (3, 1)])
        one = step(choose([1, 0, 3, 2]), relay[0])
        got_one = send(one, [(0, 1), (1, 0), (2, 3), (3, 2)])
        own = step(col, relay[1], jnp.float32)
        received = list(zip(got_one, got_mid, got_two))
        last = own[1]
    else:
        received = [[], []]
        for shift_by in range(1, ncols):
            parts = step((col + shift_by) % ncols)
            for side in range(2):
                moves = [(i, (i + shift_by) % ncols) for i in range(ncols)]
                received[side].append(lax.ppermute(parts[side], "col", moves))
        own = step(col, None, jnp.float32)
        last = own[1]

    mine = lax.dynamic_index_in_dim(roots, col, 0, keepdims=False)
    mine, _ = lax.optimization_barrier((mine, last))
    full_value = values.reshape(-1, 1)
    full_seam = seams.reshape(-1, 1)
    cauchy = full_seam / ((full_value - mine[0:1]) - mine[1:2])
    norms = jnp.sqrt(jnp.sum(cauchy * cauchy, axis=0, keepdims=True))

    out = combine(0, own[0], list(received[0]), norms, None)
    return combine(1, own[1], list(received[1]), norms, out)


def solution(mesh):
    in_specs = (P(None, "row", ("col", "depth")), P(None, ("col", "depth")), P("col"), P("col"))
    out_specs = P(None, "row", ("col", "depth"))
    return jax.shard_map(body, mesh=mesh, in_specs=in_specs, out_specs=out_specs, check_vma=False)
```
